32 devices in a mesh: data: 1 (over z), expert: 32 (over y, x, core).
Axes of the slice: x: 4, y: 4, z: 1, core: 2. Of those that a mesh axis runs over, the one named last changes fastest.
The devices are a block of a 4x4x8 slice.
Arguments:
- tokens: bfloat16 [16384, 2048], P(('data', 'expert'))
- w_router: bfloat16 [2048, 64], replicated
- routes: int32 [16384, 6], P(('data', 'expert'))
- w_gate: bfloat16 [64, 2048, 1408], P('expert')
- w_up: bfloat16 [64, 2048, 1408], P('expert')
- w_down: bfloat16 [64, 1408, 2048], P('expert')
Outputs:
- output: bfloat16 [16384, 2048], P(('data', 'expert'))
All inputs are finite; a program needn't handle non-finite values.
Results may differ from the reference program's by a relative error of at most 0.00138.
Values are sent between devices in bfloat16 or wider.
A program may use at most 768 MiB of HBM per device.

```python
import jax
import jax.numpy as jnp
from jax import lax

D = 2048
FF = 1408
EXPERTS = 64
TOP = 6
TOKENS = 512
GROUP = 32

HOT_COUNT = max(1, EXPERTS // 16)
CAP = 4 * TOKENS * TOP // EXPERTS


def draw_routing(key):
    pair_count = TOKENS * TOP
    cold_count = EXPERTS - HOT_COUNT
    cold_pairs = pair_count - HOT_COUNT * CAP
    cold_base = cold_pairs // cold_count
    cold_extra = cold_pairs - cold_base * cold_count
    key_label, key_dev = jax.random.split(key)
    labels = jax.random.permutation(key_label, EXPERTS).astype(jnp.int32)

    def one_device(dev_key):
        key_a, key_b, key_c = jax.random.split(dev_key, 3)
        jitter = jax.random.randint(key_a, (cold_count,), 0, cold_base // 2 + 1, dtype=jnp.int32)
        mixing = jax.random.permutation(key_b, cold_count)
        cold_counts = cold_base + (jnp.arange(cold_count) < cold_extra).astype(jnp.int32) + jitter - jitter[mixing]
        counts = jnp.concatenate([jnp.full((HOT_COUNT,), CAP, jnp.int32), cold_counts.astype(jnp.int32)])
        run_ends = jnp.cumsum(counts)
        position = jnp.searchsorted(run_ends, jnp.arange(pair_count, dtype=jnp.int32), side='right')
        slot_table = labels[position].reshape(TOP, TOKENS).T
        tok_order = jax.random.permutation(key_c, TOKENS)
        return slot_table[tok_order]

    dev_keys = jax.random.split(key_dev, GROUP)
    return jax.vmap(one_device)(dev_keys).reshape(GROUP * TOKENS, TOP).astype(jnp.int32)


def setup_inputs(seed: int = 0, part: int = 0) -> dict:
    key_part = jax.random.fold_in(jax.random.key(seed), part)
    key_x, key_route = jax.random.split(key_part)
    key_r, key_1, key_3, key_2 = jax.random.split(jax.random.key(seed + 1), 4)
    tokens = jax.random.normal(key_x, (GROUP * TOKENS, D), jnp.float32).astype(jnp.bfloat16)
    w_router = (jax.random.normal(key_r, (D, EXPERTS), jnp.float32) * (1.5 * D ** -0.5)).astype(jnp.bfloat16)
    routes = draw_routing(key_route)
    w_gate = (jax.random.normal(key_1, (EXPERTS, D, FF), jnp.float32) * D ** -0.5).astype(jnp.bfloat16)
    w_up = (jax.random.normal(key_3, (EXPERTS, D, FF), jnp.float32) * D ** -0.5).astype(jnp.bfloat16)
    w_down = (jax.random.normal(key_2, (EXPERTS, FF, D), jnp.float32) * FF ** -0.5).astype(jnp.bfloat16)
    return {'tokens': tokens, 'w_router': w_router, 'routes': routes, 'w_gate': w_gate, 'w_up': w_up, 'w_down': w_down}


def reference(tokens, w_router, routes, w_gate, w_up, w_down):
    row_count = tokens.shape[0]
    cap_all = GROUP * CAP
    logits = jnp.dot(tokens, w_router, preferred_element_type=jnp.float32)
    gate_vals = jax.nn.softmax(jnp.take_along_axis(logits, routes, axis=1), axis=-1)
    flat_ids = routes.reshape(-1)
    flat_gates = gate_vals.reshape(-1)
    pair_tok = jnp.arange(row_count * TOP, dtype=jnp.int32) // TOP

    def expert_step(y_acc, inputs):
        expert_id, gate_w, up_w, down_w = inputs
        hit_mask = flat_ids == expert_id
        slot_pos = jnp.where(hit_mask, jnp.cumsum(hit_mask.astype(jnp.int32)) - 1, cap_all)
        slot_tok = jnp.full((cap_all,), row_count, jnp.int32).at[slot_pos].set(pair_tok, mode='drop')
        slot_gate = jnp.zeros((cap_all,), jnp.float32).at[slot_pos].set(flat_gates, mode='drop')
        rows_in = jnp.take(tokens, slot_tok, axis=0, mode='fill', fill_value=0)
        hidden = jax.nn.silu(jnp.dot(rows_in, gate_w, preferred_element_type=jnp.float32)) * jnp.dot(rows_in, up_w, preferred_element_type=jnp.float32)
        expert_out = jnp.dot(hidden.astype(jnp.bfloat16), down_w, preferred_element_type=jnp.float32).astype(jnp.bfloat16)
        weighted = expert_out.astype(jnp.float32) * slot_gate[:, None]
        y_acc = y_acc + jax.ops.segment_sum(weighted, slot_tok, num_segments=row_count)
        return y_acc, None

    expert_ids = jnp.arange(EXPERTS, dtype=jnp.int32)
    total, _ = lax.scan(expert_step, jnp.zeros((row_count, D), jnp.float32), (expert_ids, w_gate, w_up, w_down))
    return total.astype(jnp.bfloat16)
```

```python
import functools
import math

import jax
import jax.numpy as jnp
from jax import lax
from jax.experimental import pallas as pl
from jax.experimental.pallas import tpu as pltpu
from jax.sharding import PartitionSpec as P

BF16 = jnp.bfloat16
F32 = jnp.float32
LANE = 128
CHUNK = 256
RINGS = 4
HOT = 4
SLOTS = 4
CORES = 2


def stream_kernel(side, n_real, n_all, local, sel_ref, wg, wu, wd, log, cand, recv, send,
                  cand_sem, pair_sem, recv_sem, ring_sem, log_sem, sib_sem, sib_recv_sem, credit, pair_credit):
    me = lax.axis_index('expert')
    core = me % CORES
    chip = me // CORES
    y, x = chip // side, chip % side
    sib = chip * CORES + 1 - core

    turn = ((x + y) % side) // (side - 1)
    dx = (1 - core) * (1 - turn) + core * turn
    ahead = (((y + 1 - dx) % side) * side + (x + dx) % side) * CORES + core
    turn_b = ((x + y + side - 1) % side) // (side - 1)
    dx_b = (1 - core) * (1 - turn_b) + core * turn_b
    behind = (((y + dx_b - 1 + side) % side) * side + (x + side - dx_b) % side) * CORES + core
    down = (ahead, behind)
    up = (behind, ahead)

    for k in range(HOT):
        for d in range(2):
            recv[SLOTS - 1, d, k] = jnp.zeros((CHUNK, LANE), BF16)

    barrier = pltpu.get_barrier_semaphore()
    for other in (ahead, behind, sib):
        pl.semaphore_signal(barrier, inc=1, device_id={'expert': other}, device_id_type=pl.DeviceIdType.MESH)
    pl.semaphore_wait(barrier, 3)

    per_mat = n_real // 3

    def fetch_from(p, make):
        kind = p // per_mat
        within = p % per_mat
        j, b = within // 2, within % 2

        def rows_of(w):
            for to_sib in (0, 1):
                owner_core = core if to_sib == 0 else 1 - core
                for d in range(2):
                    blk = (owner_core * 2 + d) * 2 + b
                    for le in range(local):
                        make(le, d, to_sib, w.at[le, pl.ds(pl.multiple_of(blk * CHUNK, CHUNK), CHUNK),
                                                 pl.ds(pl.multiple_of(j * LANE, LANE), LANE)], None)

        @pl.when(kind == 0)
        def _():
            rows_of(wg)

        @pl.when(kind == 1)
        def _():
            rows_of(wu)

        @pl.when(kind == 2)
        def _():
            for to_sib in (0, 1):
                owner_core = core if to_sib == 0 else 1 - core
                for d in range(2):
                    blk = (owner_core * 2 + d) * 2 + b
                    for le in range(local):
                        for part in range(2):
                            make(le, d, to_sib, wd.at[le, pl.ds(pl.multiple_of(j * LANE, LANE), LANE),
                                                      pl.ds(pl.multiple_of(blk * CHUNK + part * LANE, LANE), LANE)], part)

    def prefetch(p):
        slot = p % SLOTS

        @pl.when(p >= SLOTS)
        def _():
            pl.semaphore_wait(pair_credit, 1)
            for d in range(2):
                for le in range(local):
                    wait_pair(slot, d, le)

        def make(le, d, to_sib, src, part):
            dst = cand.at[slot, d, core * local + le]
            if part is not None:
                dst = dst.at[pl.ds(part * LANE, LANE)]
            if to_sib:
                pltpu.make_async_remote_copy(src_ref=src, dst_ref=dst, send_sem=pair_sem.at[slot, d, le],
                                             recv_sem=cand_sem.at[slot, d, core * local + le],
                                             device_id={'expert': sib}, device_id_type=pl.DeviceIdType.MESH).start()
            else:
                pltpu.make_async_copy(src, dst, cand_sem.at[slot, d, core * local + le]).start()

        fetch_from(p, make)

    def wait_pair(slot, d, le):
        one = cand.at[slot, d, core * local + le]
        pltpu.make_async_copy(one, one, pair_sem.at[slot, d, le]).wait()

    def ring_copy(slot, d, k):
        return pltpu.make_async_remote_copy(src_ref=send.at[slot, d, k], dst_ref=recv.at[slot, d, k],
                                            send_sem=ring_sem.at[slot, d, k], recv_sem=recv_sem.at[slot, d, k],
                                            device_id={'expert': down[d]}, device_id_type=pl.DeviceIdType.MESH)

    def log_copy(slot, d, s):
        return pltpu.make_async_copy(send.at[slot, d], log.at[core * 2 + d, s], log_sem.at[slot, d])

    def sib_copy(slot, d, s):
        return pltpu.make_async_remote_copy(src_ref=send.at[slot, d], dst_ref=log.at[core * 2 + d, s],
                                            send_sem=sib_sem.at[slot, d], recv_sem=sib_recv_sem.at[d],
                                            device_id={'expert': sib}, device_id_type=pl.DeviceIdType.MESH)

    def step(s, own):
        slot = s % SLOTS
        before = (s + SLOTS - 1) % SLOTS
        if own:
            @pl.when(s + 2 < n_real)
            def _():
                prefetch(s + 2)
            for d in range(2):
                for e in range(CORES * local):
                    one = cand.at[slot, d, e]
                    pltpu.make_async_copy(one, one, cand_sem.at[slot, d, e]).wait()

        @pl.when((s >= SLOTS - 1) & (s <= n_all - 2))
        def _():
            for d in range(2):
                pl.semaphore_wait(credit.at[d], 1)

        @pl.when(s >= SLOTS)
        def _():
            for d in range(2):
                log_copy(slot, d, s).wait()
                sib_copy(slot, d, s).wait_send()
                for k in range(HOT):
                    ring_copy(slot, d, k).wait_send()

        for k in range(HOT):
            for d in range(2):
                @pl.when(s >= 1)
                def _():
                    ring_copy(before, d, k).wait_recv()
                value = recv[before, d, k]
                if own:
                    pick = sel_ref[k]
                    for e in range(CORES * local):
                        value = jnp.where(pick == e + 1, cand[slot, d, e], value)
                send[slot, d, k] = value

                @pl.when(s <= n_all - 2)
                def _():
                    ring_copy(slot, d, k).start()
        for d in range(2):
            log_copy(slot, d, s).start()
            sib_copy(slot, d, s).start()

        @pl.when(s <= n_all - SLOTS - 1)
        def _():
            for d in range(2):
                pl.semaphore_signal(credit.at[d], inc=1, device_id={'expert': up[d]},
                                    device_id_type=pl.DeviceIdType.MESH)
        if own:
            @pl.when(s <= n_real - SLOTS - 1)
            def _():
                pl.semaphore_signal(pair_credit, inc=1, device_id={'expert': sib},
                                    device_id_type=pl.DeviceIdType.MESH)

    def first(p, carry):
        prefetch(p)
        return carry

    def with_own(s, carry):
        step(s, True)
        return carry

    def without_own(s, carry):
        step(s, False)
        return carry

    lax.fori_loop(0, 2, first, 0)
    lax.fori_loop(0, n_real, with_own, 0)
    lax.fori_loop(n_real, n_all, without_own, 0)

    for back in range(SLOTS):
        slot = (n_all - 1 - back) % SLOTS
        for d in range(2):
            log_copy(slot, d, 0).wait()
            sib_copy(slot, d, 0).wait_send()
            if back > 0:
                for k in range(HOT):
                    ring_copy(slot, d, k).wait_send()
        slot = (n_real - 1 - back) % SLOTS
        for d in range(2):
            for le in range(local):
                wait_pair(slot, d, le)
    for d in range(2):
        theirs = log.at[(1 - core) * 2 + d]
        pltpu.make_async_copy(theirs, theirs, sib_recv_sem.at[d]).wait()


def stream_weights(group_size, sel, w_gate, w_up, w_down):
    local, width, ff = w_gate.shape
    side = math.isqrt(group_size // CORES)
    n_real = 3 * (width // CHUNK) * (ff // LANE) // RINGS
    n_all = n_real + side * side - 1
    any_spec = pl.BlockSpec(memory_space=pl.ANY)
    return pl.pallas_call(
        functools.partial(stream_kernel, side, n_real, n_all, local),
        out_shape=jax.ShapeDtypeStruct((RINGS, n_all, HOT, CHUNK, LANE), BF16),
        in_specs=[pl.BlockSpec(memory_space=pltpu.SMEM), any_spec, any_spec, any_spec],
        out_specs=any_spec,
        scratch_shapes=[
            pltpu.VMEM((SLOTS, 2, CORES * local, CHUNK, LANE), BF16),
            pltpu.VMEM((SLOTS, 2, HOT, CHUNK, LANE), BF16),
            pltpu.VMEM((SLOTS, 2, HOT, CHUNK, LANE), BF16),
            pltpu.SemaphoreType.DMA((SLOTS, 2, CORES * local)),
            pltpu.SemaphoreType.DMA((SLOTS, 2, local)),
            pltpu.SemaphoreType.DMA((SLOTS, 2, HOT)),
            pltpu.SemaphoreType.DMA((SLOTS, 2, HOT)),
            pltpu.SemaphoreType.DMA((SLOTS, 2)),
            pltpu.SemaphoreType.DMA((SLOTS, 2)),
            pltpu.SemaphoreType.DMA((2,)),
            pltpu.SemaphoreType.REGULAR((2,)),
            pltpu.SemaphoreType.REGULAR,
        ],
        compiler_params=pltpu.CompilerParams(collective_id=1, has_side_effects=True),
        cost_estimate=pl.CostEstimate(flops=0, bytes_accessed=700_000_000, transcendentals=0),
        name='stream_weights',
    )(sel, w_gate, w_up, w_down)


def hot_kernel(parts, offs_ref, x_ref, *refs):
    gates, ups, downs = refs[:parts], refs[parts:2 * parts], refs[2 * parts:3 * parts]
    out_ref, acc = refs[3 * parts], refs[3 * parts + 1]
    j = pl.program_id(1)

    @pl.when(j == 0)
    def _():
        acc[...] = jnp.zeros_like(acc)

    ab = None
    for i in range(parts):
        both = jnp.concatenate([gates[i][...], ups[i][...]], axis=1)
        term = jnp.dot(x_ref[:, i * CHUNK:(i + 1) * CHUNK], both, preferred_element_type=F32)
        ab = term if ab is None else ab + term
    hidden = (jax.nn.silu(ab[:, :LANE]) * ab[:, LANE:]).astype(BF16)
    for i in range(parts):
        both = jnp.concatenate([downs[i][:LANE], downs[i][LANE:]], axis=1)
        acc[:, i * CHUNK:(i + 1) * CHUNK] += jnp.dot(hidden, both, preferred_element_type=F32)

    @pl.when(j == pl.num_programs(1) - 1)
    def _():
        out_ref[...] = acc[...].astype(BF16)


def hot_experts(offs, x_hot, log, ff):
    _, rows, width = x_hot.shape
    parts = width // CHUNK
    blocks = ff // LANE

    def piece(mat, i):
        ring, b = i // 2, i % 2
        return pl.BlockSpec((None, None, None, CHUNK, LANE),
                            lambda k, j, o: (ring, o[k * RINGS + ring] + mat * 2 * blocks + 2 * j + b, k, 0, 0))

    row_spec = pl.BlockSpec((None, rows, width), lambda k, j, o: (k, 0, 0))
    return pl.pallas_call(
        functools.partial(hot_kernel, parts),
        out_shape=jax.ShapeDtypeStruct((HOT, rows, width), BF16),
        grid_spec=pltpu.PrefetchScalarGridSpec(
            num_scalar_prefetch=1, grid=(HOT, blocks),
            in_specs=[row_spec] + [piece(m, i) for m in range(3) for i in range(parts)],
            out_specs=row_spec,
            scratch_shapes=[pltpu.VMEM((rows, width), F32)]),
        compiler_params=pltpu.CompilerParams(dimension_semantics=('arbitrary', 'arbitrary')),
        cost_estimate=pl.CostEstimate(flops=6 * HOT * rows * width * ff, bytes_accessed=6 * HOT * width * ff,
                                      transcendentals=0),
        name='hot_experts',
    )(offs, x_hot, *([log] * (3 * parts)))


def split3(v):
    hi = lax.reduce_precision(v, 8, 7)
    mid = lax.reduce_precision(v - hi, 8, 7)
    low = lax.reduce_precision(v - hi - mid, 8, 7)
    return [hi.astype(BF16), mid.astype(BF16), low.astype(BF16)]


def weighted(pos, cap, gate_parts, rows):
    toks, count = pos.shape
    hit = pos[:, :, None] == jnp.arange(cap, dtype=jnp.int32)[None, None, :]
    mats = [jnp.where(hit, g[:, :, None], jnp.zeros((), BF16)).reshape(toks, count * cap) for g in gate_parts]
    out = jnp.dot(jnp.concatenate(mats, axis=0), rows, preferred_element_type=F32)
    return out[:toks] + out[toks:2 * toks] + out[2 * toks:]


def solution(mesh):
    group_size = mesh.shape['expert']
    row_spec = P(('data', 'expert'), None)
    expert_spec = P('expert', None, None)
    side = math.isqrt(group_size // CORES)
    ring_len = side * side

    def device_step(tokens, w_router, routes, w_gate, w_up, w_down):
        toks, width = tokens.shape
        picks = routes.shape[1]
        experts = w_router.shape[1]
        local, _, ff = w_gate.shape
        capacity = 4 * toks * picks // experts
        cold_cap = capacity // 3
        hot_cap = capacity - cold_cap

        logits = jnp.dot(tokens, w_router, preferred_element_type=F32)
        ids = jnp.arange(experts, dtype=jnp.int32)
        mask = jnp.any(routes[:, :, None] == ids[None, None, :], axis=1)
        top = jnp.max(jnp.where(mask, logits, -jnp.inf), axis=1, keepdims=True)
        raised = jnp.where(mask, jnp.exp(logits - top), 0.0)
        gates = raised / jnp.sum(raised, axis=1, keepdims=True)
        gate_parts = split3(gates)

        order = jnp.arange(toks, dtype=jnp.int32)
        earlier = (order[None, :] < order[:, None]).astype(BF16)
        rank = jnp.dot(earlier, mask.astype(BF16), preferred_element_type=F32).astype(jnp.int32)
        pos = jnp.where(mask, rank, -1)
        counts = jnp.sum(mask.astype(jnp.int32), axis=0)

        pos_t = pos.T.reshape(group_size, local, toks)
        slots = jnp.arange(cold_cap, dtype=jnp.int32)
        received = []
        for le in range(local):
            pick_rows = (pos_t[:, le, None, :] == slots[None, :, None]).astype(BF16).reshape(group_size * cold_cap, toks)
            rows = jnp.dot(pick_rows, tokens, preferred_element_type=F32).astype(BF16)
            received.append(lax.all_to_all(rows.reshape(group_size, cold_cap, width), 'expert', 0, 0, tiled=True)
                            .reshape(group_size * cold_cap, width))

        most = lax.pmax(counts, 'expert')
        is_hot = most > cold_cap
        hot_place = jnp.cumsum(is_hot.astype(jnp.int32)) - 1
        n_hot = jnp.sum(is_hot.astype(jnp.int32))
        my_chip = lax.axis_index('expert') // CORES
        my_y, my_x = my_chip // side, my_chip % side
        ring_a = side * my_y + (my_x + my_y) % side
        ring_b = side * my_x + (my_x + my_y) % side

        def hot_pass(batch):
            want = batch * HOT + jnp.arange(HOT, dtype=jnp.int32)
            match = is_hot[None, :] & (hot_place[None, :] == want[:, None])
            there = jnp.any(match, axis=1)
            hot_id = jnp.sum(jnp.where(match, ids[None, :], 0), axis=1)
            chip = hot_id // (local * CORES)
            sel = jnp.where(there & (chip == my_chip), 1 + hot_id % (local * CORES), 0)
            cy, cx = chip // side, chip % side
            root_a = side * cy + (cx + cy) % side
            root_b = side * cx + (cx + cy) % side
            offs = jnp.stack([(ring_a - root_a) % ring_len, (root_a - ring_a) % ring_len,
                              (ring_b - root_b) % ring_len, (root_b - ring_b) % ring_len], axis=1).reshape(-1)
            log = stream_weights(group_size, sel, w_gate, w_up, w_down)
            col = jnp.sum(jnp.where(match[:, None, :], pos[None, :, :] - cold_cap, 0), axis=2)
            col = jnp.where(there[:, None], col, -1)
            hit = (col[:, None, :] == jnp.arange(hot_cap, dtype=jnp.int32)[None, :, None]).astype(BF16)
            x_hot = jnp.dot(hit.reshape(HOT * hot_cap, toks), tokens, preferred_element_type=F32).astype(BF16)
            o_hot = hot_experts(offs, x_hot.reshape(HOT, hot_cap, width), log, ff)
            g_hot = jnp.sum(jnp.where(match[:, None, :], gates[None, :, :], 0.0), axis=2)
            return weighted(col.T, hot_cap, split3(g_hot.T), o_hot.reshape(HOT * hot_cap, width))

        total = hot_pass(jnp.int32(0))
        for le in range(local):
            rows = received[le]
            hidden = jax.nn.silu(jnp.dot(rows, w_gate[le], preferred_element_type=F32)) * jnp.dot(
                rows, w_up[le], preferred_element_type=F32)
            out = jnp.dot(hidden.astype(BF16), w_down[le], preferred_element_type=F32).astype(BF16)
            back = lax.all_to_all(out.reshape(group_size, cold_cap, width), 'expert', 0, 0, tiled=True)
            pos_le = pos.reshape(toks, group_size, local)[:, :, le]
            total = total + weighted(pos_le, cold_cap, [g.reshape(toks, group_size, local)[:, :, le] for g in gate_parts],
                                     back.reshape(group_size * cold_cap, width))

        def more(state):
            return state[0] * HOT < n_hot

        def again(state):
            return state[0] + 1, state[1] + hot_pass(state[0])

        _, total = lax.while_loop(more, again, (jnp.int32(1), total))
        return total.astype(BF16)

    return jax.shard_map(device_step, mesh=mesh,
                         in_specs=(row_spec, P(None, None), row_spec, expert_spec, expert_spec, expert_spec),
                         out_specs=row_spec, check_vma=False)
```
